32 devices in a mesh: dp: 8 (over z, x), rep: 4 (over y, core).
Axes of the slice: x: 2, y: 2, z: 4, core: 2. Of those that a mesh axis runs over, the one named last changes fastest.
Arguments:
- features: bfloat16 [5120, 8192], P('dp', 'rep'), may hold values from -6 to 6
- out_grads: bfloat16 [5120, 1024], P('dp'), may hold values from -12 to 12, as said below
- cold_sums: bfloat16 [8, 8192, 1024], P('dp', 'rep'), may hold values from -96 to 96
- weight: float32 [8192, 1024], P(('rep', 'dp')), may hold values from -3 to 3
- moment: float32 [8192, 1024], P(('rep', 'dp')), may hold values from -6 to 6
- second: float32 [8192, 1024], P(('rep', 'dp')), may hold values from 0.01 to 4
- ranks: int32 [8], replicated, may hold values from 0 to 7, each once
Outputs:
- new_weight: float32 [8192, 1024], P(('rep', 'dp'))
- new_moment: float32 [8192, 1024], P(('rep', 'dp'))
- new_second: float32 [8192, 1024], P(('rep', 'dp'))
- new_cold: bfloat16 [8, 8192, 1024], P('dp', 'rep')
- column_sq: float32 [1024], replicated
The draws below stay inside these ranges and needn't reach their ends.
Inputs may be any that keep to these rules, and one draw needn't show every extreme that they name: `ranks`: each block number appears once. `out_grads`: column scales differ from column to column.
All inputs are finite; a program needn't handle non-finite values.
Results may differ from the reference program's by a relative error of at most 0.001.
Values sent between devices are 32-bit elements; how exact they have to be, the bound alone decides.
A program may use at most 128 MiB of HBM per device.

```python
import math
import jax
import jax.numpy as jnp
from jax import lax

D = 8192
C = 1024
TOK_DEV = 640
BLOCK = 128
NB = 8
HOT = 4
TOKENS = 5120
N_DP = 8


def draw_out_grads(key, part):
    first, second_key = jax.random.split(key, 2)
    base = jax.random.normal(first, (TOKENS, C), jnp.float32)
    col_scale = jnp.exp(jax.random.uniform(second_key, (1, C), jnp.float32, -1.4, 1.4))
    values = base * col_scale
    return jnp.clip(values, -12.0, 12.0).astype(jnp.bfloat16)


def level_of(key, shape, pieces, smallest, high):
    level, own = 1.0, jax.random.fold_in(key, 6)
    for position, shards_of in pieces:
        heights = jnp.exp(jax.random.uniform(jax.random.fold_in(own, position), (shards_of,), jnp.float32, smallest / len(pieces), high / len(pieces)))
        level = level * jnp.repeat(heights, shape[position] // shards_of).reshape([-1 if axis == position else 1 for axis in range(len(shape))])
    return level


def centred(key, dims, width, bound, cuts=(), dtype=jnp.bfloat16):
    gain = level_of(key, dims, cuts, -0.22, 0.18) if cuts else 1.0
    result = jax.random.normal(key, dims, jnp.float32) * width * gain
    return jnp.minimum(jnp.maximum(result, -bound), bound).astype(dtype)


def setup_inputs(seed: int = 0) -> dict:
    keys = jax.random.split(jax.random.key(seed), 8)
    return {
        "features": centred(keys[0], (TOKENS, D), 1.0, 6.0, ((0, 8), (1, 4))),
        "out_grads": draw_out_grads(jax.random.fold_in(keys[7], 71), 0),
        "cold_sums": centred(keys[2], (N_DP, D, C), 16.0, 96.0, ((0, 8), (1, 4))),
        "weight": centred(keys[3], (D, C), 0.5, 3.0, ((0, 32),), jnp.float32),
        "moment": centred(keys[4], (D, C), 1.0, 6.0, ((0, 32),), jnp.float32),
        "second": jnp.clip(jnp.exp(math.log(4.0) - 5.9914646 * jax.random.uniform(keys[5], (D, C), jnp.float32) ** level_of(keys[5], (D, C), ((0, 32),), -0.2, 0.2)), 0.01, 4.0),
        "ranks": jax.random.permutation(keys[6], NB).astype(jnp.int32),
    }


def reference(features, out_grads, cold_sums, weight, moment, second, ranks):
    hot_block = ranks < HOT
    hot_col = jnp.repeat(hot_block, BLOCK)
    feats = features.reshape(N_DP, TOK_DEV, D)
    grads = out_grads.reshape(N_DP, TOK_DEV, C)

    def one_group(carry, inputs):
        summed, squares = carry
        feat, cot, cold = inputs
        local = cold.astype(jnp.float32) + jnp.dot(feat.T, cot, preferred_element_type=jnp.float32)
        kept = jnp.where(hot_col[None, :], jnp.float32(0.0), local).astype(jnp.bfloat16)
        return ((summed + local, squares + lax.optimization_barrier(jnp.sum(local * local, axis=0))), kept)
    start = (jnp.zeros((D, C), jnp.float32), jnp.zeros((C,), jnp.float32))
    (summed, column_sq), new_cold = lax.scan(one_group, start, (feats, grads, cold_sums))
    rms = jnp.sqrt(column_sq / jnp.float32(D * N_DP * TOK_DEV))
    clip = 1.0 / jnp.maximum(jnp.float32(1.0), rms)
    grad_mean = summed * clip[None, :] / jnp.float32(N_DP)
    moved = 0.9 * moment + 0.1 * grad_mean
    squared = 0.95 * second + 0.05 * grad_mean * grad_mean
    step_size = 0.05 * (moved / (1.0 - 0.9 ** 10)) / (jnp.sqrt(squared / (1.0 - 0.95 ** 10)) + 1e-08)
    new_moment = jnp.where(hot_col[None, :], moved, moment)
    new_second = jnp.where(hot_col[None, :], squared, second)
    new_weight = jnp.where(hot_col[None, :], weight - step_size, weight)
    return (new_weight, new_moment, new_second, new_cold, column_sq)
```

```python
import functools
import jax
import jax.numpy as jnp
from jax import lax
from jax.experimental import pallas as pl
from jax.experimental.pallas import tpu as pltpu
from jax.sharding import PartitionSpec as P

LANES = 128
SUB = 2
VMEM_GRANT = 30 * 2**20
MESH = pl.DeviceIdType.MESH


def bits_of(size):
    return max(size.bit_length() - 1, 0)


def flipped(index, bit):
    step = 1 << bit
    return index + step - 2 * step * ((index // step) % 2)


def exchange_kernel(
    n, reps, hot,
    ranks, feat, og, cold, weight, moment, second,
    summed, sq_out, nc_out, w_out, m_out, s_out,
    feat_v, og_v, cold_v, local, pack, rx, lbuf, rbuf, hsrc, hbuf,
    in_sem, state_sem, send1, recv1, zsend, lrecv, rrecv, hsend, hrecv,
):
    m = n // 2
    rows, width = cold.shape[1], cold.shape[2]
    blocks = width // LANES
    own = rows // n
    chunk = max(own, LANES)
    chunks = rows // chunk
    part = own // SUB
    me = lax.axis_index("dp")
    rep = lax.axis_index("rep")
    x = me % 2
    p = me // 2
    partner = me + 1 - 2 * x
    dp_bits, rep_bits = bits_of(n), bits_of(reps)
    steps = [("dp", b) for b in range(dp_bits)] + [("rep", b) for b in range(rep_bits)]

    half = max(m // 2, 1)
    flip = p // half if m > 1 else 0
    pr = p + flip * (m - 1 - 2 * p)

    def dest(k):
        if m == 1:
            return 0 * k
        late = (k + pr) // (m - 1)
        near = (1 - late) * (m - 1 - k) + late * (k + pr - (m - 1))
        last = k // (m - 1)
        near = (1 - last) * near + last * pr
        return near + flip * (m - 1 - 2 * near)

    def chunk_at(i):
        if chunk != own:
            return i
        k = i % m
        side = i // m
        return 2 * dest(k) + (1 - side) * (1 - x) + side * x

    def hop(axis, b):
        index = me if axis == "dp" else rep
        return {axis: flipped(index, b)}

    barrier = pltpu.get_barrier_semaphore()
    pl.semaphore_signal(barrier, inc=1, device_id={"dp": partner}, device_id_type=MESH)

    @pl.when(p > 0)
    def _():
        pl.semaphore_signal(barrier, inc=1, device_id={"dp": me - 2}, device_id_type=MESH)

    @pl.when(p < m - 1)
    def _():
        pl.semaphore_signal(barrier, inc=1, device_id={"dp": me + 2}, device_id_type=MESH)

    for axis, b in steps[1:]:
        pl.semaphore_signal(barrier, inc=1, device_id=hop(axis, b), device_id_type=MESH)

    def feat_copy(i):
        c = chunk_at(i)
        cols = pl.ds(pl.multiple_of(c * chunk, LANES), chunk)
        return pltpu.make_async_copy(feat.at[:, cols], feat_v.at[i], in_sem.at[0, i])

    def cold_copy(i):
        c = chunk_at(i)
        at = pl.ds(pl.multiple_of(c * chunk, LANES), chunk)
        return pltpu.make_async_copy(cold.at[0, at], cold_v.at[i], in_sem.at[1, i])

    state = [
        pltpu.make_async_copy(src, dst, state_sem.at[i])
        for i, (src, dst) in enumerate(
            ((weight, w_out), (moment, m_out), (second, s_out), (og, og_v))
        )
    ]
    feat_copy(0).start()
    state[3].start()
    cold_copy(0).start()

    def fetch(i, carry):
        feat_copy(i).start()
        cold_copy(i).start()
        return carry

    lax.fori_loop(1, chunks, fetch, 0)
    for copy in state[:3]:
        copy.start()

    hsrc[0] = jnp.zeros_like(hsrc[0])
    keep = [
        jnp.minimum(jnp.maximum(ranks[b] - (hot - 1), 0), 1).astype(jnp.float32)
        for b in range(blocks)
    ]
    picks = []
    for s in range(hot):
        row = []
        for b in range(blocks):
            gap = ranks[b] - s
            row.append((1 - jnp.minimum(gap * gap, 1)).astype(jnp.float32))
        picks.append(row)

    def cross(k, sub):
        d = dest(k)
        src = pl.ds(pl.multiple_of((2 * d + 1 - x) * own + sub * part, 8), part)
        dst = pl.ds(pl.multiple_of(d * own + sub * part, 8), part)
        return pltpu.make_async_remote_copy(
            src_ref=pack.at[src], dst_ref=rx.at[dst],
            send_sem=send1.at[d, sub], recv_sem=recv1.at[d, sub],
            device_id={"dp": partner}, device_id_type=MESH,
        )

    def along(d, sub, right):
        src = pl.ds(pl.multiple_of((2 * d + x) * own + sub * part, 8), part)
        dst = pl.ds(pl.multiple_of(d * own + sub * part, 8), part)
        return pltpu.make_async_remote_copy(
            src_ref=pack.at[src], dst_ref=(lbuf if right else rbuf).at[dst],
            send_sem=zsend.at[d, sub], recv_sem=(lrecv if right else rrecv).at[d, sub],
            device_id={"dp": me + 2 if right else me - 2}, device_id_type=MESH,
        )

    def norm_copy(s):
        return pltpu.make_async_remote_copy(
            src_ref=hsrc.at[s], dst_ref=hbuf.at[s],
            send_sem=hsend.at[s], recv_sem=hrecv.at[s],
            device_id=hop(*steps[s]), device_id_type=MESH,
        )

    greeted = 1 + (len(steps) - 1) + (p + m - 1) // m + (2 * m - 2 - p) // m
    pl.semaphore_wait(barrier, greeted)
    state[3].wait()

    def compute(i, carry):
        c = chunk_at(i)
        feat_copy(i).wait()
        cold_copy(i).wait()
        local[...] = lax.dot_general(
            feat_v[i], og_v[...], (((0,), (0,)), ((), ())),
            preferred_element_type=jnp.float32,
        ) + cold_v[i].astype(jnp.float32)
        at = pl.ds(pl.multiple_of(c * chunk, LANES), chunk)
        for s in range(hot):
            picked = local[:, :LANES] * picks[s][0]
            for b in range(1, blocks):
                picked += local[:, b * LANES:(b + 1) * LANES] * picks[s][b]
            pack[at, s * LANES:(s + 1) * LANES] = picked
        if chunk == own:
            @pl.when(i < m)
            def _():
                for sub in range(SUB):
                    cross(i % m, sub).start()
        for b in range(blocks):
            cols = slice(b * LANES, (b + 1) * LANES)
            values = local[:, cols]
            hsrc[0, b:b + 1, :] += jnp.sum(values * values, axis=0, keepdims=True)
            nc_out[0, at, cols] = (values * keep[b]).astype(jnp.bfloat16)
        return carry

    lax.fori_loop(0, chunks, compute, 0)
    if chunk != own:
        def launch(k, carry):
            for sub in range(SUB):
                cross(k, sub).start()
            return carry

        lax.fori_loop(0, m, launch, 0)
    norm_copy(0).start()

    def process(k, sub):
        d = dest(k)
        mine = pl.ds(pl.multiple_of((2 * d + x) * own + sub * part, 8), part)
        slot = pl.ds(pl.multiple_of(d * own + sub * part, 8), part)
        cross(k, sub).wait_recv()
        pack[mine] += rx[slot]

        @pl.when(jnp.logical_and(d >= p, p > 0))
        def _():
            along(d, sub, True).wait_recv()
            pack[mine] += lbuf[slot]

        @pl.when(jnp.logical_and(d <= p, p < m - 1))
        def _():
            along(d, sub, False).wait_recv()
            pack[mine] += rbuf[slot]

        @pl.when(d > p)
        def _():
            along(d, sub, True).start()

        @pl.when(d < p)
        def _():
            along(d, sub, False).start()

        @pl.when(d == p)
        def _():
            summed[sub * part:(sub + 1) * part] = pack[mine]

    def norm_step(s):
        norm_copy(s).wait_recv()
        hsrc[s + 1] = hsrc[s] + hbuf[s]
        if s + 1 < len(steps):
            norm_copy(s + 1).start()

    done = 0
    if m <= 8:
        for k in range(m):
            for sub in range(SUB):
                if done < len(steps):
                    norm_step(done)
                    done += 1
                process(k, sub)
    else:
        def walk(k, carry):
            for sub in range(SUB):
                process(k, sub)
            return carry

        lax.fori_loop(0, m, walk, 0)
    for s in range(done, len(steps)):
        norm_step(s)
    sq_out[...] = hsrc[len(steps)]

    for copy in state[:3]:
        copy.wait()

    def drain(k, carry):
        d = dest(k)
        for sub in range(SUB):
            cross(k, sub).wait_send()

            @pl.when(d > p)
            def _():
                along(d, sub, True).wait_send()

            @pl.when(d < p)
            def _():
                along(d, sub, False).wait_send()
        return carry

    lax.fori_loop(0, m, drain, 0)
    for s in range(len(steps)):
        norm_copy(s).wait_send()


def update_kernel(
    n, total_rows, tokens, hot,
    ranks, summed, sq, nc, weight, moment, second,
    w_hbm, m_hbm, s_hbm, nc_hbm,
    fresh, nc_sem, sem,
):
    rows, width = weight.shape
    blocks = width // LANES
    cold_out = pltpu.make_async_copy(nc, nc_hbm, nc_sem)
    cold_out.start()
    for b in range(blocks):
        cols = slice(b * LANES, (b + 1) * LANES)
        slot = ranks[b]

        @pl.when(slot < hot)
        def _():
            total = sq[b:b + 1, :]
            rms = jnp.sqrt(total / jnp.float32(total_rows * n * tokens))
            clip = 1.0 / jnp.maximum(jnp.float32(1.0), rms)
            at = pl.ds(pl.multiple_of(slot * LANES, LANES), LANES)
            grad = summed[:, at] * clip / jnp.float32(n)
            moved = 0.9 * moment[:, cols] + 0.1 * grad
            squared = 0.95 * second[:, cols] + 0.05 * grad * grad
            fresh[1, :, cols] = moved
            fresh[2, :, cols] = squared
            step = 0.05 * (moved / (1.0 - 0.9**10)) / (
                jnp.sqrt(squared / (1.0 - 0.95**10)) + 1e-08
            )
            fresh[0, :, cols] = weight[:, cols] - step

        @pl.when(slot >= hot)
        def _():
            fresh[0, :, cols] = weight[:, cols]
            fresh[1, :, cols] = moment[:, cols]
            fresh[2, :, cols] = second[:, cols]

    copies = [
        pltpu.make_async_copy(fresh.at[i], dst, sem.at[i])
        for i, dst in enumerate((w_hbm, m_hbm, s_hbm))
    ]
    for copy in copies:
        copy.start()
    for copy in copies:
        copy.wait()
    cold_out.wait()


def body(n, reps, features, out_grads, cold_sums, weight, moment, second, ranks):
    tokens, rows = features.shape
    width = out_grads.shape[1]
    blocks = ranks.shape[0]
    hot = blocks // 2
    packed = hot * LANES
    m = n // 2
    own = rows // n
    chunk = max(own, LANES)
    chunks = rows // chunk
    hops = bits_of(n) + bits_of(reps)
    f32, bf16 = jnp.float32, jnp.bfloat16
    vmem = pl.BlockSpec(memory_space=pltpu.VMEM)
    smem = pl.BlockSpec(memory_space=pltpu.SMEM)
    hbm = pl.BlockSpec(memory_space=pl.ANY)
    dma = pltpu.SemaphoreType.DMA
    summed, sq, kept, w, mo, se = pl.pallas_call(
        functools.partial(exchange_kernel, n, reps, hot),
        out_shape=(
            pltpu.VMEM((own, packed), f32),
            pltpu.VMEM((blocks, LANES), f32),
            pltpu.VMEM(cold_sums.shape, bf16),
            pltpu.VMEM(weight.shape, f32),
            pltpu.VMEM(weight.shape, f32),
            pltpu.VMEM(weight.shape, f32),
        ),
        in_specs=[smem] + [pl.BlockSpec(memory_space=pltpu.HBM)] * 6,
        out_specs=(vmem,) * 6,
        scratch_shapes=[
            pltpu.VMEM((chunks, tokens, chunk), bf16),
            pltpu.VMEM((tokens, width), bf16),
            pltpu.VMEM((chunks, chunk, width), bf16),
            pltpu.VMEM((chunk, width), f32),
            pltpu.VMEM((rows, packed), f32),
            pltpu.VMEM((m * own, packed), f32),
            pltpu.VMEM((m * own, packed), f32),
            pltpu.VMEM((m * own, packed), f32),
            pltpu.VMEM((hops + 1, blocks, LANES), f32),
            pltpu.VMEM((hops, blocks, LANES), f32),
            dma((2, chunks)),
            dma((4,)),
            dma((m, SUB)),
            dma((m, SUB)),
            dma((m, SUB)),
            dma((m, SUB)),
            dma((m, SUB)),
            dma((hops,)),
            dma((hops,)),
        ],
        compiler_params=pltpu.CompilerParams(
            collective_id=0, has_side_effects=True, vmem_limit_bytes=VMEM_GRANT
        ),
        name="exchange",
    )(ranks, features, out_grads, cold_sums, weight, moment, second)
    new_weight, new_moment, new_second, new_cold = pl.pallas_call(
        functools.partial(update_kernel, n, rows * reps, tokens, hot),
        out_shape=(
            jax.ShapeDtypeStruct(weight.shape, f32),
            jax.ShapeDtypeStruct(weight.shape, f32),
            jax.ShapeDtypeStruct(weight.shape, f32),
            jax.ShapeDtypeStruct(cold_sums.shape, bf16),
        ),
        in_specs=[smem] + [vmem] * 6,
        out_specs=(hbm,) * 4,
        scratch_shapes=[pltpu.VMEM((3,) + weight.shape, f32), dma, dma((3,))],
        compiler_params=pltpu.CompilerParams(vmem_limit_bytes=VMEM_GRANT),
        name="update",
    )(ranks, summed, sq, kept, w, mo, se)
    return new_weight, new_moment, new_second, new_cold, sq.reshape(width)


def solution(mesh):
    owned = P(("rep", "dp"), None)
    placed = (P("dp", "rep"), P("dp", None), P("dp", "rep", None), owned, owned, owned, P())
    return jax.shard_map(
        functools.partial(body, mesh.shape["dp"], mesh.shape["rep"]),
        mesh=mesh,
        in_specs=placed,
        out_specs=(owned, owned, owned, P("dp", "rep", None), P()),
        check_vma=False,
    )
```

```python
import functools
import jax
import jax.numpy as jnp
from jax import lax
from jax.experimental import pallas as pl
from jax.experimental.pallas import tpu as pltpu
from jax.sharding import PartitionSpec as P

LANES = 128
SUB = 2
VMEM_GRANT = 30 * 2**20
EXCHANGE_GRANT = 55 * 2**20
MESH = pl.DeviceIdType.MESH


def bits_of(size):
    return max(size.bit_length() - 1, 0)


def flipped(index, bit):
    step = 1 << bit
    return index + step - 2 * step * ((index // step) % 2)


def exchange_kernel(
    n, reps, hot,
    ranks, feat, og, cold, weight, moment, second,
    summed, sq_out, nc_out, w_out, m_out, s_out,
    feat_v, og_v, cold_v, local, pack, rx, lbuf, rbuf, hsrc, hbuf, gbuf,
    in_sem, state_sem, send1, recv1, zsend, lrecv, rrecv, hsend, hrecv, gsend, grecv,
):
    m = n // 2
    rows, width = cold.shape[1], cold.shape[2]
    blocks = width // LANES
    own = rows // n
    chunk = max(own, LANES)
    chunks = rows // chunk
    part = own // SUB
    me = lax.axis_index("dp")
    rep = lax.axis_index("rep")
    x = me % 2
    p = me // 2
    partner = me + 1 - 2 * x
    rep_bits = bits_of(reps)

    half = max(m // 2, 1)
    flip = p // half if m > 1 else 0
    pr = p + flip * (m - 1 - 2 * p)

    def dest(k):
        if m == 1:
            return 0 * k
        late = (k + pr) // (m - 1)
        near = (1 - late) * (m - 1 - k) + late * (k + pr - (m - 1))
        last = k // (m - 1)
        near = (1 - last) * near + last * pr
        return near + flip * (m - 1 - 2 * near)

    def chunk_at(i):
        if chunk != own:
            return i
        k = i % m
        side = i // m
        return 2 * dest(k) + (1 - side) * (1 - x) + side * x

    barrier = pltpu.get_barrier_semaphore()

    def peer(o):
        return (me + o) % n

    def greet(o, carry):
        pl.semaphore_signal(barrier, inc=1, device_id={"dp": peer(o)}, device_id_type=MESH)
        return carry

    lax.fori_loop(1, n, greet, 0)
    for b in range(rep_bits):
        pl.semaphore_signal(
            barrier, inc=1, device_id={"rep": flipped(rep, b)}, device_id_type=MESH
        )

    def feat_copy(i):
        c = chunk_at(i)
        cols = pl.ds(pl.multiple_of(c * chunk, LANES), chunk)
        return pltpu.make_async_copy(feat.at[:, cols], feat_v.at[i], in_sem.at[0, i])

    def cold_copy(i):
        c = chunk_at(i)
        at = pl.ds(pl.multiple_of(c * chunk, LANES), chunk)
        return pltpu.make_async_copy(cold.at[0, at], cold_v.at[i], in_sem.at[1, i])

    state = [
        pltpu.make_async_copy(src, dst, state_sem.at[i])
        for i, (src, dst) in enumerate(
            ((weight, w_out), (moment, m_out), (second, s_out), (og, og_v))
        )
    ]
    feat_copy(0).start()
    state[3].start()
    cold_copy(0).start()

    def fetch(i, carry):
        feat_copy(i).start()
        cold_copy(i).start()
        return carry

    lax.fori_loop(1, chunks, fetch, 0)
    for copy in state[:3]:
        copy.start()

    hsrc[0] = jnp.zeros_like(hsrc[0])
    keep = [
        jnp.minimum(jnp.maximum(ranks[b] - (hot - 1), 0), 1).astype(jnp.float32)
        for b in range(blocks)
    ]
    picks = []
    for s in range(hot):
        row = []
        for b in range(blocks):
            gap = ranks[b] - s
            row.append((1 - jnp.minimum(gap * gap, 1)).astype(jnp.float32))
        picks.append(row)

    def cross(k, sub):
        d = dest(k)
        src = pl.ds(pl.multiple_of((2 * d + 1 - x) * own + sub * part, 8), part)
        dst = pl.ds(pl.multiple_of(d * own + sub * part, 8), part)
        return pltpu.make_async_remote_copy(
            src_ref=pack.at[src], dst_ref=rx.at[dst],
            send_sem=send1.at[d, sub], recv_sem=recv1.at[d, sub],
            device_id={"dp": partner}, device_id_type=MESH,
        )

    def along(d, sub, right):
        src = pl.ds(pl.multiple_of((2 * d + x) * own + sub * part, 8), part)
        dst = pl.ds(pl.multiple_of(d * own + sub * part, 8), part)
        return pltpu.make_async_remote_copy(
            src_ref=pack.at[src], dst_ref=(lbuf if right else rbuf).at[dst],
            send_sem=zsend.at[d, sub], recv_sem=(lrecv if right else rrecv).at[d, sub],
            device_id={"dp": me + 2 if right else me - 2}, device_id_type=MESH,
        )

    def norm_copy(s):
        return pltpu.make_async_remote_copy(
            src_ref=hsrc.at[s], dst_ref=hbuf.at[s],
            send_sem=hsend.at[s], recv_sem=hrecv.at[s],
            device_id={"rep": flipped(rep, s)}, device_id_type=MESH,
        )

    def spread_copy(o):
        return pltpu.make_async_remote_copy(
            src_ref=gbuf.at[me], dst_ref=gbuf.at[me],
            send_sem=gsend.at[o], recv_sem=grecv.at[me],
            device_id={"dp": peer(o)}, device_id_type=MESH,
        )

    def arrival(j):
        return pltpu.make_async_remote_copy(
            src_ref=gbuf.at[j], dst_ref=gbuf.at[j],
            send_sem=gsend.at[0], recv_sem=grecv.at[j],
            device_id={"dp": partner}, device_id_type=MESH,
        )

    pl.semaphore_wait(barrier, n - 1 + rep_bits)
    state[3].wait()

    def compute(i, carry):
        c = chunk_at(i)
        feat_copy(i).wait()
        cold_copy(i).wait()
        local[...] = lax.dot_general(
            feat_v[i], og_v[...], (((0,), (0,)), ((), ())),
            preferred_element_type=jnp.float32,
        ) + cold_v[i].astype(jnp.float32)
        at = pl.ds(pl.multiple_of(c * chunk, LANES), chunk)
        for s in range(hot):
            picked = local[:, :LANES] * picks[s][0]
            for b in range(1, blocks):
                picked += local[:, b * LANES:(b + 1) * LANES] * picks[s][b]
            pack[at, s * LANES:(s + 1) * LANES] = picked
        if chunk == own:
            @pl.when(i < m - 1)
            def _():
                for sub in range(SUB):
                    cross(i % m, sub).start()
        for b in range(blocks):
            cols = slice(b * LANES, (b + 1) * LANES)
            values = local[:, cols]
            hsrc[0, b:b + 1, :] += jnp.sum(values * values, axis=0, keepdims=True)
            nc_out[0, at, cols] = (values * keep[b]).astype(jnp.bfloat16)
        return carry

    lax.fori_loop(0, chunks, compute, 0)
    if chunk != own:
        def launch(k, carry):
            for sub in range(SUB):
                cross(k, sub).start()
            return carry

        lax.fori_loop(0, m - 1, launch, 0)
    if rep_bits:
        norm_copy(0).start()

    def process(k, sub):
        d = dest(k)
        mine = pl.ds(pl.multiple_of((2 * d + x) * own + sub * part, 8), part)
        slot = pl.ds(pl.multiple_of(d * own + sub * part, 8), part)
        cross(k, sub).wait_recv()
        pack[mine] += rx[slot]

        @pl.when(jnp.logical_and(d >= p, p > 0))
        def _():
            along(d, sub, True).wait_recv()
            pack[mine] += lbuf[slot]

        @pl.when(jnp.logical_and(d <= p, p < m - 1))
        def _():
            along(d, sub, False).wait_recv()
            pack[mine] += rbuf[slot]

        @pl.when(d > p)
        def _():
            along(d, sub, True).start()

        @pl.when(d < p)
        def _():
            along(d, sub, False).start()

        @pl.when(d == p)
        def _():
            summed[sub * part:(sub + 1) * part] = pack[mine]

    def norm_step(s):
        if s < rep_bits:
            norm_copy(s).wait_recv()
            hsrc[s + 1] = hsrc[s] + hbuf[s]
            if s + 1 < rep_bits:
                norm_copy(s + 1).start()
        if s == max(rep_bits, 1) - 1:
            gbuf[me] = hsrc[rep_bits]

            def spread(o, carry):
                spread_copy(o).start()
                return carry

            lax.fori_loop(1, n, spread, 0)
            for sub in range(SUB):
                cross(m - 1, sub).start()

    done = 0
    norm_steps = max(rep_bits, 1)
    if m == 1:
        for s in range(norm_steps):
            norm_step(s)
        done = norm_steps
    for k in range(min(m, 2)):
        for sub in range(SUB):
            process(k, sub)
            if done < norm_steps:
                norm_step(done)
                done += 1
    for s in range(done, norm_steps):
        norm_step(s)

    def walk(k, carry):
        for sub in range(SUB):
            process(k, sub)
        return carry

    lax.fori_loop(min(m, 2), m, walk, 0)

    def gather(o, carry):
        arrival(peer(o)).wait_recv()
        return carry

    lax.fori_loop(1, n, gather, 0)

    sq_out[...] = gbuf[0]

    def total(j, carry):
        sq_out[...] += gbuf[j]
        return carry

    lax.fori_loop(1, n, total, 0)

    for copy in state[:3]:
        copy.wait()

    def drain(k, carry):
        d = dest(k)
        for sub in range(SUB):
            cross(k, sub).wait_send()

            @pl.when(d > p)
            def _():
                along(d, sub, True).wait_send()

            @pl.when(d < p)
            def _():
                along(d, sub, False).wait_send()
        return carry

    lax.fori_loop(0, m, drain, 0)
    for s in range(rep_bits):
        norm_copy(s).wait_send()

    def settle(o, carry):
        spread_copy(o).wait_send()
        return carry

    lax.fori_loop(1, n, settle, 0)


def update_kernel(
    n, total_rows, tokens, hot,
    ranks, summed, sq, nc, weight, moment, second,
    w_hbm, m_hbm, s_hbm, nc_hbm,
    fresh, nc_sem, sem,
):
    rows, width = weight.shape
    blocks = width // LANES
    cold_out = pltpu.make_async_copy(nc, nc_hbm, nc_sem)
    cold_out.start()
    for b in range(blocks):
        cols = slice(b * LANES, (b + 1) * LANES)
        slot = ranks[b]

        @pl.when(slot < hot)
        def _():
            total = sq[b:b + 1, :]
            rms = jnp.sqrt(total / jnp.float32(total_rows * n * tokens))
            clip = 1.0 / jnp.maximum(jnp.float32(1.0), rms)
            at = pl.ds(pl.multiple_of(slot * LANES, LANES), LANES)
            grad = summed[:, at] * clip / jnp.float32(n)
            moved = 0.9 * moment[:, cols] + 0.1 * grad
            squared = 0.95 * second[:, cols] + 0.05 * grad * grad
            fresh[1, :, cols] = moved
            fresh[2, :, cols] = squared
            step = 0.05 * (moved / (1.0 - 0.9**10)) / (
                jnp.sqrt(squared / (1.0 - 0.95**10)) + 1e-08
            )
            fresh[0, :, cols] = weight[:, cols] - step

        @pl.when(slot >= hot)
        def _():
            fresh[0, :, cols] = weight[:, cols]
            fresh[1, :, cols] = moment[:, cols]
            fresh[2, :, cols] = second[:, cols]

    copies = [
        pltpu.make_async_copy(fresh.at[i], dst, sem.at[i])
        for i, dst in enumerate((w_hbm, m_hbm, s_hbm))
    ]
    for copy in copies:
        copy.start()
    for copy in copies:
        copy.wait()
    cold_out.wait()


def body(n, reps, features, out_grads, cold_sums, weight, moment, second, ranks):
    tokens, rows = features.shape
    width = out_grads.shape[1]
    blocks = ranks.shape[0]
    hot = blocks // 2
    packed = hot * LANES
    m = n // 2
    own = rows // n
    chunk = max(own, LANES)
    chunks = rows // chunk
    hops = max(bits_of(reps), 1)
    f32, bf16 = jnp.float32, jnp.bfloat16
    vmem = pl.BlockSpec(memory_space=pltpu.VMEM)
    smem = pl.BlockSpec(memory_space=pltpu.SMEM)
    hbm = pl.BlockSpec(memory_space=pl.ANY)
    dma = pltpu.SemaphoreType.DMA
    summed, sq, kept, w, mo, se = pl.pallas_call(
        functools.partial(exchange_kernel, n, reps, hot),
        out_shape=(
            pltpu.VMEM((own, packed), f32),
            pltpu.VMEM((blocks, LANES), f32),
            pltpu.VMEM(cold_sums.shape, bf16),
            pltpu.VMEM(weight.shape, f32),
            pltpu.VMEM(weight.shape, f32),
            pltpu.VMEM(weight.shape, f32),
        ),
        in_specs=[smem] + [pl.BlockSpec(memory_space=pltpu.HBM)] * 6,
        out_specs=(vmem,) * 6,
        scratch_shapes=[
            pltpu.VMEM((chunks, tokens, chunk), bf16),
            pltpu.VMEM((tokens, width), bf16),
            pltpu.VMEM((chunks, chunk, width), bf16),
            pltpu.VMEM((chunk, width), f32),
            pltpu.VMEM((rows, packed), f32),
            pltpu.VMEM((m * own, packed), f32),
            pltpu.VMEM((m * own, packed), f32),
            pltpu.VMEM((m * own, packed), f32),
            pltpu.VMEM((hops + 1, blocks, LANES), f32),
            pltpu.VMEM((hops, blocks, LANES), f32),
            pltpu.VMEM((n, blocks, LANES), f32),
            dma((2, chunks)),
            dma((4,)),
            dma((m, SUB)),
            dma((m, SUB)),
            dma((m, SUB)),
            dma((m, SUB)),
            dma((m, SUB)),
            dma((hops,)),
            dma((hops,)),
            dma((n,)),
            dma((n,)),
        ],
        compiler_params=pltpu.CompilerParams(
            collective_id=0, has_side_effects=True, vmem_limit_bytes=EXCHANGE_GRANT
        ),
        name="exchange",
    )(ranks, features, out_grads, cold_sums, weight, moment, second)
    new_weight, new_moment, new_second, new_cold = pl.pallas_call(
        functools.partial(update_kernel, n, rows * reps, tokens, hot),
        out_shape=(
            jax.ShapeDtypeStruct(weight.shape, f32),
            jax.ShapeDtypeStruct(weight.shape, f32),
            jax.ShapeDtypeStruct(weight.shape, f32),
            jax.ShapeDtypeStruct(cold_sums.shape, bf16),
        ),
        in_specs=[smem] + [vmem] * 6,
        out_specs=(hbm,) * 4,
        scratch_shapes=[pltpu.VMEM((3,) + weight.shape, f32), dma, dma((3,))],
        compiler_params=pltpu.CompilerParams(vmem_limit_bytes=VMEM_GRANT),
        name="update",
    )(ranks, summed, sq, kept, w, mo, se)
    return new_weight, new_moment, new_second, new_cold, sq.reshape(width)


def solution(mesh):
    owned = P(("rep", "dp"), None)
    placed = (P("dp", "rep"), P("dp", None), P("dp", "rep", None), owned, owned, owned, P())
    return jax.shard_map(
        functools.partial(body, mesh.shape["dp"], mesh.shape["rep"]),
        mesh=mesh,
        in_specs=placed,
        out_specs=(owned, owned, owned, P("dp", "rep", None), P()),
        check_vma=False,
    )
```

```python
import functools
import jax
import jax.numpy as jnp
from jax import lax
from jax.experimental import pallas as pl
from jax.experimental.pallas import tpu as pltpu
from jax.sharding import PartitionSpec as P

LANES = 128
SUB = 2
VMEM_GRANT = 30 * 2**20
EXCHANGE_GRANT = 55 * 2**20
MESH = pl.DeviceIdType.MESH


def bits_of(size):
    return max(size.bit_length() - 1, 0)


def split_rows(own):
    late = max(own * 5 // 32 // 8, 1) * 8
    early = own - late
    cuts = [early * i // SUB // 8 * 8 for i in range(SUB)] + [early]
    return early, late, cuts


def flipped(index, bit):
    step = 1 << bit
    return index + step - 2 * step * ((index // step) % 2)


def exchange_kernel(
    n, reps, hot,
    ranks, feat, og, cold, weight, moment, second,
    summed, sq_out, nc_out, w_out, m_out, s_out,
    feat_v, og_v, cold_v, local, pack, rx, lbuf, rbuf, packz, rxz, lbufz, rbufz, hsrc, hbuf, gbuf,
    in_sem, state_sem, send1, recv1, zsend, lrecv, rrecv, hsend, hrecv, gsend, grecv,
    zzsend, zzleft, zzright, zxsend, zxrecv,
):
    m = n // 2
    rows, width = cold.shape[1], cold.shape[2]
    blocks = width // LANES
    own = rows // n
    chunk = max(own, LANES)
    chunks = rows // chunk
    early, late, cuts = split_rows(own)
    group = chunk // own
    me = lax.axis_index("dp")
    rep = lax.axis_index("rep")
    x = me % 2
    p = me // 2
    partner = me + 1 - 2 * x
    rep_bits = bits_of(reps)

    half = max(m // 2, 1)
    flip = p // half if m > 1 else 0
    pr = p + flip * (m - 1 - 2 * p)

    def dest(k):
        if m == 1:
            return 0 * k
        late = (k + pr) // (m - 1)
        near = (1 - late) * (m - 1 - k) + late * (k + pr - (m - 1))
        last = k // (m - 1)
        near = (1 - last) * near + last * pr
        return near + flip * (m - 1 - 2 * near)

    def chunk_at(i):
        if chunk != own:
            return i
        k = i // 2
        side = i % 2
        return 2 * dest(k) + (1 - side) * (1 - x) + side * x

    barrier = pltpu.get_barrier_semaphore()

    def peer(o):
        return (me + o) % n

    def greet(o, carry):
        pl.semaphore_signal(barrier, inc=1, device_id={"dp": peer(o)}, device_id_type=MESH)
        return carry

    lax.fori_loop(1, n, greet, 0)
    for b in range(rep_bits):
        pl.semaphore_signal(
            barrier, inc=1, device_id={"rep": flipped(rep, b)}, device_id_type=MESH
        )

    def feat_copy(i):
        c = chunk_at(i)
        cols = pl.ds(pl.multiple_of(c * chunk, LANES), chunk)
        return pltpu.make_async_copy(feat.at[:, cols], feat_v.at[i], in_sem.at[0, i])

    def cold_copy(i):
        c = chunk_at(i)
        at = pl.ds(pl.multiple_of(c * chunk, LANES), chunk)
        return pltpu.make_async_copy(cold.at[0, at], cold_v.at[i], in_sem.at[1, i])

    state = [
        pltpu.make_async_copy(src, dst, state_sem.at[i])
        for i, (src, dst) in enumerate(
            ((weight, w_out), (moment, m_out), (second, s_out), (og, og_v))
        )
    ]
    feat_copy(0).start()
    state[3].start()
    cold_copy(0).start()

    def fetch(i, carry):
        feat_copy(i).start()
        cold_copy(i).start()
        return carry

    lax.fori_loop(1, chunks, fetch, 0)
    for copy in state[:3]:
        copy.start()

    hsrc[0] = jnp.zeros_like(hsrc[0])
    keep = [
        jnp.minimum(jnp.maximum(ranks[b] - (hot - 1), 0), 1).astype(jnp.float32)
        for b in range(blocks)
    ]
    picks = []
    for s in range(hot):
        row = []
        for b in range(blocks):
            gap = ranks[b] - s
            row.append((1 - jnp.minimum(gap * gap, 1)).astype(jnp.float32))
        picks.append(row)

    def rows_of(index, sub):
        return pl.ds(pl.multiple_of(index * early + cuts[sub], 8), cuts[sub + 1] - cuts[sub])

    def cross(k, sub):
        d = dest(k)
        return pltpu.make_async_remote_copy(
            src_ref=pack.at[rows_of(2 * d + 1 - x, sub)], dst_ref=rx.at[rows_of(d, sub)],
            send_sem=send1.at[d, sub], recv_sem=recv1.at[d, sub],
            device_id={"dp": partner}, device_id_type=MESH,
        )

    def along(d, sub, right):
        return pltpu.make_async_remote_copy(
            src_ref=pack.at[rows_of(2 * d + x, sub)],
            dst_ref=(lbuf if right else rbuf).at[rows_of(d, sub)],
            send_sem=zsend.at[d, sub], recv_sem=(lrecv if right else rrecv).at[d, sub],
            device_id={"dp": me + 2 if right else me - 2}, device_id_type=MESH,
        )

    def whole_along(d, right):
        return pltpu.make_async_remote_copy(
            src_ref=packz.at[d], dst_ref=(lbufz if right else rbufz).at[d],
            send_sem=zzsend.at[d], recv_sem=(zzleft if right else zzright).at[d],
            device_id={"dp": me + 2 if right else me - 2}, device_id_type=MESH,
        )

    def whole_cross():
        return pltpu.make_async_remote_copy(
            src_ref=packz.at[p, pl.ds(pl.multiple_of((1 - x) * late, 8), late)],
            dst_ref=rxz, send_sem=zxsend, recv_sem=zxrecv,
            device_id={"dp": partner}, device_id_type=MESH,
        )

    def whole_step(k):
        d = dest(k)

        @pl.when(jnp.logical_and(d >= p, p > 0))
        def _():
            whole_along(d, True).wait_recv()
            packz[d] += lbufz[d]

        @pl.when(jnp.logical_and(d <= p, p < m - 1))
        def _():
            whole_along(d, False).wait_recv()
            packz[d] += rbufz[d]

        @pl.when(d > p)
        def _():
            whole_along(d, True).start()

        @pl.when(d < p)
        def _():
            whole_along(d, False).start()

    def norm_copy(s):
        return pltpu.make_async_remote_copy(
            src_ref=hsrc.at[s], dst_ref=hbuf.at[s],
            send_sem=hsend.at[s], recv_sem=hrecv.at[s],
            device_id={"rep": flipped(rep, s)}, device_id_type=MESH,
        )

    def spread_copy(o):
        return pltpu.make_async_remote_copy(
            src_ref=gbuf.at[me], dst_ref=gbuf.at[me],
            send_sem=gsend.at[o], recv_sem=grecv.at[me],
            device_id={"dp": peer(o)}, device_id_type=MESH,
        )

    def arrival(j):
        return pltpu.make_async_remote_copy(
            src_ref=gbuf.at[j], dst_ref=gbuf.at[j],
            send_sem=gsend.at[0], recv_sem=grecv.at[j],
            device_id={"dp": partner}, device_id_type=MESH,
        )

    pl.semaphore_wait(barrier, n - 1 + rep_bits)
    state[3].wait()

    def compute(i, carry):
        c = chunk_at(i)
        feat_copy(i).wait()
        cold_copy(i).wait()
        local[...] = lax.dot_general(
            feat_v[i], og_v[...], (((0,), (0,)), ((), ())),
            preferred_element_type=jnp.float32,
        ) + cold_v[i].astype(jnp.float32)
        at = pl.ds(pl.multiple_of(c * chunk, LANES), chunk)
        for s in range(hot):
            picked = local[:, :LANES] * picks[s][0]
            for b in range(1, blocks):
                picked += local[:, b * LANES:(b + 1) * LANES] * picks[s][b]
            lanes = slice(s * LANES, (s + 1) * LANES)
            for g in range(group):
                j = c * group + g
                top = g * own
                pack[pl.ds(pl.multiple_of(j * early, 8), early), lanes] = (
                    picked[top:top + early]
                )
                packz[j // 2, pl.ds(pl.multiple_of(j % 2 * late, 8), late), lanes] = (
                    picked[top + early:top + own]
                )
        if chunk == own:
            @pl.when(jnp.logical_and(i < chunks - 2, i % 2 == 0))
            def _():
                for sub in range(SUB):
                    cross(i // 2, sub).start()

        for b in range(blocks):
            cols = slice(b * LANES, (b + 1) * LANES)
            values = local[:, cols]
            hsrc[0, b:b + 1, :] += jnp.sum(values * values, axis=0, keepdims=True)
            nc_out[0, at, cols] = (values * keep[b]).astype(jnp.bfloat16)
        if chunk == own:
            @pl.when(jnp.logical_and(i < chunks - 2, i % 2 == 1))
            def _():
                whole_step(i // 2)

        return carry

    lax.fori_loop(0, chunks, compute, 0)
    if chunk != own:
        def launch(k, carry):
            for sub in range(SUB):
                cross(k, sub).start()
            whole_step(k)
            return carry

        lax.fori_loop(0, m - 1, launch, 0)
    if rep_bits:
        norm_copy(0).start()

    def process(k, sub):
        d = dest(k)
        mine = rows_of(2 * d + x, sub)
        slot = rows_of(d, sub)
        cross(k, sub).wait_recv()
        pack[mine] += rx[slot]

        @pl.when(jnp.logical_and(d >= p, p > 0))
        def _():
            along(d, sub, True).wait_recv()
            pack[mine] += lbuf[slot]

        @pl.when(jnp.logical_and(d <= p, p < m - 1))
        def _():
            along(d, sub, False).wait_recv()
            pack[mine] += rbuf[slot]

        @pl.when(d > p)
        def _():
            along(d, sub, True).start()

        @pl.when(d < p)
        def _():
            along(d, sub, False).start()

        @pl.when(d == p)
        def _():
            summed[cuts[sub]:cuts[sub + 1]] = pack[mine]

    def norm_step(s):
        if s < rep_bits:
            norm_copy(s).wait_recv()
            hsrc[s + 1] = hsrc[s] + hbuf[s]
            if s + 1 < rep_bits:
                norm_copy(s + 1).start()
        if s == max(rep_bits, 1) - 1:
            gbuf[me] = hsrc[rep_bits]

            def spread(o, carry):
                spread_copy(o).start()
                return carry

            lax.fori_loop(1, n, spread, 0)
            for sub in range(SUB):
                cross(m - 1, sub).start()

    done = 0
    norm_steps = max(rep_bits, 1)
    if m == 1:
        for s in range(norm_steps):
            norm_step(s)
        done = norm_steps
    for k in range(min(m, 2)):
        for sub in range(SUB):
            process(k, sub)
            if done < norm_steps:
                norm_step(done)
                done += 1
    for s in range(done, norm_steps):
        norm_step(s)

    def walk(k, carry):
        for sub in range(SUB):
            process(k, sub)
        return carry

    whole_step(m - 1)
    whole_cross().start()
    lax.fori_loop(min(m, 2), m, walk, 0)
    whole_cross().wait_recv()
    summed[early:own] = packz[p, pl.ds(pl.multiple_of(x * late, 8), late)] + rxz[...]

    def gather(o, carry):
        arrival(peer(o)).wait_recv()
        return carry

    lax.fori_loop(1, n, gather, 0)

    sq_out[...] = gbuf[0]

    def total(j, carry):
        sq_out[...] += gbuf[j]
        return carry

    lax.fori_loop(1, n, total, 0)

    for copy in state[:3]:
        copy.wait()

    def drain(k, carry):
        d = dest(k)
        for sub in range(SUB):
            cross(k, sub).wait_send()

            @pl.when(d > p)
            def _():
                along(d, sub, True).wait_send()

            @pl.when(d < p)
            def _():
                along(d, sub, False).wait_send()
        return carry

    lax.fori_loop(0, m, drain, 0)
    whole_cross().wait_send()

    def drain_whole(k, carry):
        d = dest(k)

        @pl.when(d > p)
        def _():
            whole_along(d, True).wait_send()

        @pl.when(d < p)
        def _():
            whole_along(d, False).wait_send()
        return carry

    lax.fori_loop(0, m, drain_whole, 0)
    for s in range(rep_bits):
        norm_copy(s).wait_send()

    def settle(o, carry):
        spread_copy(o).wait_send()
        return carry

    lax.fori_loop(1, n, settle, 0)


def update_kernel(
    n, total_rows, tokens, hot,
    ranks, summed, sq, nc, weight, moment, second,
    w_hbm, m_hbm, s_hbm, nc_hbm,
    fresh, nc_sem, sem,
):
    rows, width = weight.shape
    blocks = width // LANES
    cold_out = pltpu.make_async_copy(nc, nc_hbm, nc_sem)
    cold_out.start()
    for b in range(blocks):
        cols = slice(b * LANES, (b + 1) * LANES)
        slot = ranks[b]

        @pl.when(slot < hot)
        def _():
            total = sq[b:b + 1, :]
            rms = jnp.sqrt(total / jnp.float32(total_rows * n * tokens))
            clip = 1.0 / jnp.maximum(jnp.float32(1.0), rms)
            at = pl.ds(pl.multiple_of(slot * LANES, LANES), LANES)
            grad = summed[:, at] * clip / jnp.float32(n)
            moved = 0.9 * moment[:, cols] + 0.1 * grad
            squared = 0.95 * second[:, cols] + 0.05 * grad * grad
            fresh[1, :, cols] = moved
            fresh[2, :, cols] = squared
            step = 0.05 * (moved / (1.0 - 0.9**10)) / (
                jnp.sqrt(squared / (1.0 - 0.95**10)) + 1e-08
            )
            fresh[0, :, cols] = weight[:, cols] - step

        @pl.when(slot >= hot)
        def _():
            fresh[0, :, cols] = weight[:, cols]
            fresh[1, :, cols] = moment[:, cols]
            fresh[2, :, cols] = second[:, cols]

    copies = [
        pltpu.make_async_copy(fresh.at[i], dst, sem.at[i])
        for i, dst in enumerate((w_hbm, m_hbm, s_hbm))
    ]
    for copy in copies:
        copy.start()
    for copy in copies:
        copy.wait()
    cold_out.wait()


def body(n, reps, features, out_grads, cold_sums, weight, moment, second, ranks):
    tokens, rows = features.shape
    width = out_grads.shape[1]
    blocks = ranks.shape[0]
    hot = blocks // 2
    packed = hot * LANES
    m = n // 2
    own = rows // n
    chunk = max(own, LANES)
    chunks = rows // chunk
    early, late, _ = split_rows(own)
    hops = max(bits_of(reps), 1)
    f32, bf16 = jnp.float32, jnp.bfloat16
    vmem = pl.BlockSpec(memory_space=pltpu.VMEM)
    smem = pl.BlockSpec(memory_space=pltpu.SMEM)
    hbm = pl.BlockSpec(memory_space=pl.ANY)
    dma = pltpu.SemaphoreType.DMA
    summed, sq, kept, w, mo, se = pl.pallas_call(
        functools.partial(exchange_kernel, n, reps, hot),
        out_shape=(
            pltpu.VMEM((own, packed), f32),
            pltpu.VMEM((blocks, LANES), f32),
            pltpu.VMEM(cold_sums.shape, bf16),
            pltpu.VMEM(weight.shape, f32),
            pltpu.VMEM(weight.shape, f32),
            pltpu.VMEM(weight.shape, f32),
        ),
        in_specs=[smem] + [pl.BlockSpec(memory_space=pltpu.HBM)] * 6,
        out_specs=(vmem,) * 6,
        scratch_shapes=[
            pltpu.VMEM((chunks, tokens, chunk), bf16),
            pltpu.VMEM((tokens, width), bf16),
            pltpu.VMEM((chunks, chunk, width), bf16),
            pltpu.VMEM((chunk, width), f32),
            pltpu.VMEM((n * early, packed), f32),
            pltpu.VMEM((m * early, packed), f32),
            pltpu.VMEM((m * early, packed), f32),
            pltpu.VMEM((m * early, packed), f32),
            pltpu.VMEM((m, 2 * late, packed), f32),
            pltpu.VMEM((late, packed), f32),
            pltpu.VMEM((m, 2 * late, packed), f32),
            pltpu.VMEM((m, 2 * late, packed), f32),
            pltpu.VMEM((hops + 1, blocks, LANES), f32),
            pltpu.VMEM((hops, blocks, LANES), f32),
            pltpu.VMEM((n, blocks, LANES), f32),
            dma((2, chunks)),
            dma((4,)),
            dma((m, SUB)),
            dma((m, SUB)),
            dma((m, SUB)),
            dma((m, SUB)),
            dma((m, SUB)),
            dma((hops,)),
            dma((hops,)),
            dma((n,)),
            dma((n,)),
            dma((m,)),
            dma((m,)),
            dma((m,)),
            dma,
            dma,
        ],
        compiler_params=pltpu.CompilerParams(
            collective_id=0, has_side_effects=True, vmem_limit_bytes=EXCHANGE_GRANT
        ),
        name="exchange",
    )(ranks, features, out_grads, cold_sums, weight, moment, second)
    new_weight, new_moment, new_second, new_cold = pl.pallas_call(
        functools.partial(update_kernel, n, rows * reps, tokens, hot),
        out_shape=(
            jax.ShapeDtypeStruct(weight.shape, f32),
            jax.ShapeDtypeStruct(weight.shape, f32),
            jax.ShapeDtypeStruct(weight.shape, f32),
            jax.ShapeDtypeStruct(cold_sums.shape, bf16),
        ),
        in_specs=[smem] + [vmem] * 6,
        out_specs=(hbm,) * 4,
        scratch_shapes=[pltpu.VMEM((3,) + weight.shape, f32), dma, dma((3,))],
        compiler_params=pltpu.CompilerParams(vmem_limit_bytes=VMEM_GRANT),
        name="update",
    )(ranks, summed, sq, kept, w, mo, se)
    return new_weight, new_moment, new_second, new_cold, sq.reshape(width)


def solution(mesh):
    owned = P(("rep", "dp"), None)
    placed = (P("dp", "rep"), P("dp", None), P("dp", "rep", None), owned, owned, owned, P())
    return jax.shard_map(
        functools.partial(body, mesh.shape["dp"], mesh.shape["rep"]),
        mesh=mesh,
        in_specs=placed,
        out_specs=(owned, owned, owned, P("dp", "rep", None), P()),
        check_vma=False,
    )
```

```python
import functools
import jax
import jax.numpy as jnp
from jax import lax
from jax.experimental import pallas as pl
from jax.experimental.pallas import tpu as pltpu
from jax.sharding import PartitionSpec as P

LANES = 128
SUB = 2
VMEM_GRANT = 30 * 2**20
EXCHANGE_GRANT = 55 * 2**20
MESH = pl.DeviceIdType.MESH


def bits_of(size):
    return max(size.bit_length() - 1, 0)


def split_rows(own):
    late = max(own * 3 // 32 // 8, 1) * 8
    early = own - late
    cuts = [early * i // SUB // 8 * 8 for i in range(SUB)] + [early]
    return early, late, cuts


def flipped(index, bit):
    step = 1 << bit
    return index + step - 2 * step * ((index // step) % 2)


def exchange_kernel(
    n, reps, hot,
    ranks, feat, og, cold, weight, moment, second,
    summed, sq_out, nc_out, w_out, m_out, s_out,
    feat_v, og_v, cold_v, local, pack, rx, lbuf, rbuf, packz, rxz, lbufz, rbufz, hsrc, hbuf, gbuf,
    in_sem, state_sem, send1, recv1, zsend, lrecv, rrecv, hsend, hrecv, gsend, grecv,
    zzsend, zzleft, zzright, zxsend, zxrecv,
):
    m = n // 2
    rows, width = cold.shape[1], cold.shape[2]
    blocks = width // LANES
    own = rows // n
    chunk = max(own, LANES)
    chunks = rows // chunk
    early, late, cuts = split_rows(own)
    group = chunk // own
    me = lax.axis_index("dp")
    rep = lax.axis_index("rep")
    x = me % 2
    p = me // 2
    partner = me + 1 - 2 * x
    rep_bits = bits_of(reps)

    half = max(m // 2, 1)
    flip = p // half if m > 1 else 0
    pr = p + flip * (m - 1 - 2 * p)

    def dest(k):
        if m == 1:
            return 0 * k
        late = (k + pr) // (m - 1)
        near = (1 - late) * (m - 1 - k) + late * (k + pr - (m - 1))
        last = k // (m - 1)
        near = (1 - last) * near + last * pr
        return near + flip * (m - 1 - 2 * near)

    def chunk_at(i):
        if chunk != own:
            return i
        k = i // 2
        side = i % 2
        return 2 * dest(k) + (1 - side) * (1 - x) + side * x

    barrier = pltpu.get_barrier_semaphore()

    def peer(o):
        return (me + o) % n

    def greet(o, carry):
        pl.semaphore_signal(barrier, inc=1, device_id={"dp": peer(o)}, device_id_type=MESH)
        return carry

    lax.fori_loop(1, n, greet, 0)
    for b in range(rep_bits):
        pl.semaphore_signal(
            barrier, inc=1, device_id={"rep": flipped(rep, b)}, device_id_type=MESH
        )

    def feat_copy(i):
        c = chunk_at(i)
        cols = pl.ds(pl.multiple_of(c * chunk, LANES), chunk)
        return pltpu.make_async_copy(feat.at[:, cols], feat_v.at[i], in_sem.at[0, i])

    def cold_copy(i):
        c = chunk_at(i)
        at = pl.ds(pl.multiple_of(c * chunk, LANES), chunk)
        return pltpu.make_async_copy(cold.at[0, at], cold_v.at[i], in_sem.at[1, i])

    state = [
        pltpu.make_async_copy(src, dst, state_sem.at[i])
        for i, (src, dst) in enumerate(
            ((weight, w_out), (moment, m_out), (second, s_out), (og, og_v))
        )
    ]
    feat_copy(0).start()
    state[3].start()
    cold_copy(0).start()

    def fetch(i, carry):
        feat_copy(i).start()
        cold_copy(i).start()
        return carry

    lax.fori_loop(1, chunks, fetch, 0)
    for copy in state[:3]:
        copy.start()

    hsrc[0] = jnp.zeros_like(hsrc[0])
    keep = [
        jnp.minimum(jnp.maximum(ranks[b] - (hot - 1), 0), 1).astype(jnp.float32)
        for b in range(blocks)
    ]
    picks = []
    for s in range(hot):
        row = []
        for b in range(blocks):
            gap = ranks[b] - s
            row.append((1 - jnp.minimum(gap * gap, 1)).astype(jnp.float32))
        picks.append(row)

    def rows_of(index, sub):
        return pl.ds(pl.multiple_of(index * early + cuts[sub], 8), cuts[sub + 1] - cuts[sub])

    def cross(k, sub):
        d = dest(k)
        return pltpu.make_async_remote_copy(
            src_ref=pack.at[rows_of(2 * d + 1 - x, sub)], dst_ref=rx.at[rows_of(d, sub)],
            send_sem=send1.at[d, sub], recv_sem=recv1.at[d, sub],
            device_id={"dp": partner}, device_id_type=MESH,
        )

    def along(d, sub, right):
        return pltpu.make_async_remote_copy(
            src_ref=pack.at[rows_of(2 * d + x, sub)],
            dst_ref=(lbuf if right else rbuf).at[rows_of(d, sub)],
            send_sem=zsend.at[d, sub], recv_sem=(lrecv if right else rrecv).at[d, sub],
            device_id={"dp": me + 2 if right else me - 2}, device_id_type=MESH,
        )

    def whole_along(d, right):
        return pltpu.make_async_remote_copy(
            src_ref=packz.at[d], dst_ref=(lbufz if right else rbufz).at[d],
            send_sem=zzsend.at[d], recv_sem=(zzleft if right else zzright).at[d],
            device_id={"dp": me + 2 if right else me - 2}, device_id_type=MESH,
        )

    def whole_cross():
        return pltpu.make_async_remote_copy(
            src_ref=packz.at[p, pl.ds(pl.multiple_of((1 - x) * late, 8), late)],
            dst_ref=rxz, send_sem=zxsend, recv_sem=zxrecv,
            device_id={"dp": partner}, device_id_type=MESH,
        )

    def whole_step(k):
        d = dest(k)

        @pl.when(jnp.logical_and(d >= p, p > 0))
        def _():
            whole_along(d, True).wait_recv()
            packz[d] += lbufz[d]

        @pl.when(jnp.logical_and(d <= p, p < m - 1))
        def _():
            whole_along(d, False).wait_recv()
            packz[d] += rbufz[d]

        @pl.when(d > p)
        def _():
            whole_along(d, True).start()

        @pl.when(d < p)
        def _():
            whole_along(d, False).start()

    def norm_copy(s):
        return pltpu.make_async_remote_copy(
            src_ref=hsrc.at[s], dst_ref=hbuf.at[s],
            send_sem=hsend.at[s], recv_sem=hrecv.at[s],
            device_id={"rep": flipped(rep, s)}, device_id_type=MESH,
        )

    def spread_copy(o):
        return pltpu.make_async_remote_copy(
            src_ref=gbuf.at[me], dst_ref=gbuf.at[me],
            send_sem=gsend.at[o], recv_sem=grecv.at[me],
            device_id={"dp": peer(o)}, device_id_type=MESH,
        )

    def arrival(j):
        return pltpu.make_async_remote_copy(
            src_ref=gbuf.at[j], dst_ref=gbuf.at[j],
            send_sem=gsend.at[0], recv_sem=grecv.at[j],
            device_id={"dp": partner}, device_id_type=MESH,
        )

    pl.semaphore_wait(barrier, n - 1 + rep_bits)
    state[3].wait()

    def compute(i, carry):
        c = chunk_at(i)
        feat_copy(i).wait()
        cold_copy(i).wait()
        local[...] = lax.dot_general(
            feat_v[i], og_v[...], (((0,), (0,)), ((), ())),
            preferred_element_type=jnp.float32,
        ) + cold_v[i].astype(jnp.float32)
        at = pl.ds(pl.multiple_of(c * chunk, LANES), chunk)
        for s in range(hot):
            picked = local[:, :LANES] * picks[s][0]
            for b in range(1, blocks):
                picked += local[:, b * LANES:(b + 1) * LANES] * picks[s][b]
            lanes = slice(s * LANES, (s + 1) * LANES)
            for g in range(group):
                j = c * group + g
                top = g * own
                pack[pl.ds(pl.multiple_of(j * early, 8), early), lanes] = (
                    picked[top:top + early]
                )
                packz[j // 2, pl.ds(pl.multiple_of(j % 2 * late, 8), late), lanes] = (
                    picked[top + early:top + own]
                )
        if chunk == own:
            @pl.when(jnp.logical_and(i < chunks - 2, i % 2 == 0))
            def _():
                for sub in range(SUB):
                    cross(i // 2, sub).start()

        for b in range(blocks):
            cols = slice(b * LANES, (b + 1) * LANES)
            values = local[:, cols]
            hsrc[0, b:b + 1, :] += jnp.sum(values * values, axis=0, keepdims=True)
            nc_out[0, at, cols] = (values * keep[b]).astype(jnp.bfloat16)
        if chunk == own:
            @pl.when(jnp.logical_and(i < chunks - 2, i % 2 == 1))
            def _():
                whole_step(i // 2)

        return carry

    lax.fori_loop(0, chunks, compute, 0)
    if chunk != own:
        def launch(k, carry):
            for sub in range(SUB):
                cross(k, sub).start()
            whole_step(k)
            return carry

        lax.fori_loop(0, m - 1, launch, 0)
    if rep_bits:
        norm_copy(0).start()

    def process(k, sub):
        d = dest(k)
        mine = rows_of(2 * d + x, sub)
        slot = rows_of(d, sub)
        cross(k, sub).wait_recv()
        pack[mine] += rx[slot]

        @pl.when(jnp.logical_and(d >= p, p > 0))
        def _():
            along(d, sub, True).wait_recv()
            pack[mine] += lbuf[slot]

        @pl.when(jnp.logical_and(d <= p, p < m - 1))
        def _():
            along(d, sub, False).wait_recv()
            pack[mine] += rbuf[slot]

        @pl.when(d > p)
        def _():
            along(d, sub, True).start()

        @pl.when(d < p)
        def _():
            along(d, sub, False).start()

        @pl.when(d == p)
        def _():
            summed[cuts[sub]:cuts[sub + 1]] = pack[mine]

    def norm_step(s):
        if s < rep_bits:
            norm_copy(s).wait_recv()
            hsrc[s + 1] = hsrc[s] + hbuf[s]
            if s + 1 < rep_bits:
                norm_copy(s + 1).start()
        if s == max(rep_bits, 1) - 1:
            gbuf[me] = hsrc[rep_bits]

            def spread(o, carry):
                spread_copy(o).start()
                return carry

            lax.fori_loop(1, n, spread, 0)
            for sub in range(SUB):
                cross(m - 1, sub).start()

    done = 0
    norm_steps = max(rep_bits, 1)
    if m == 1:
        for s in range(norm_steps):
            norm_step(s)
        done = norm_steps
    for k in range(min(m, 2)):
        for sub in range(SUB):
            process(k, sub)
            if done < norm_steps:
                norm_step(done)
                done += 1
    for s in range(done, norm_steps):
        norm_step(s)

    def walk(k, carry):
        for sub in range(SUB):
            process(k, sub)
        return carry

    whole_step(m - 1)
    whole_cross().start()
    lax.fori_loop(min(m, 2), m, walk, 0)
    whole_cross().wait_recv()
    summed[early:own] = packz[p, pl.ds(pl.multiple_of(x * late, 8), late)] + rxz[...]

    def gather(o, carry):
        arrival(peer(o)).wait_recv()
        return carry

    lax.fori_loop(1, n, gather, 0)

    sq_out[...] = gbuf[0]

    def total(j, carry):
        sq_out[...] += gbuf[j]
        return carry

    lax.fori_loop(1, n, total, 0)

    for copy in state[:3]:
        copy.wait()

    def drain(k, carry):
        d = dest(k)
        for sub in range(SUB):
            cross(k, sub).wait_send()

            @pl.when(d > p)
            def _():
                along(d, sub, True).wait_send()

            @pl.when(d < p)
            def _():
                along(d, sub, False).wait_send()
        return carry

    lax.fori_loop(0, m, drain, 0)
    whole_cross().wait_send()

    def drain_whole(k, carry):
        d = dest(k)

        @pl.when(d > p)
        def _():
            whole_along(d, True).wait_send()

        @pl.when(d < p)
        def _():
            whole_along(d, False).wait_send()
        return carry

    lax.fori_loop(0, m, drain_whole, 0)
    for s in range(rep_bits):
        norm_copy(s).wait_send()

    def settle(o, carry):
        spread_copy(o).wait_send()
        return carry

    lax.fori_loop(1, n, settle, 0)


def update_kernel(
    n, total_rows, tokens, hot,
    ranks, summed, sq, nc, weight, moment, second,
    w_hbm, m_hbm, s_hbm, nc_hbm, sq_hbm,
    fresh, nc_sem, sq_sem, sem,
):
    rows, width = weight.shape
    blocks = width // LANES
    cold_out = pltpu.make_async_copy(nc, nc_hbm, nc_sem)
    cold_out.start()
    sq_out = pltpu.make_async_copy(sq, sq_hbm, sq_sem)
    sq_out.start()
    for b in range(blocks):
        cols = slice(b * LANES, (b + 1) * LANES)
        slot = ranks[b]

        @pl.when(slot < hot)
        def _():
            total = sq[b:b + 1, :]
            rms = jnp.sqrt(total / jnp.float32(total_rows * n * tokens))
            clip = 1.0 / jnp.maximum(jnp.float32(1.0), rms)
            at = pl.ds(pl.multiple_of(slot * LANES, LANES), LANES)
            grad = summed[:, at] * clip / jnp.float32(n)
            moved = 0.9 * moment[:, cols] + 0.1 * grad
            squared = 0.95 * second[:, cols] + 0.05 * grad * grad
            fresh[1, :, cols] = moved
            fresh[2, :, cols] = squared
            step = 0.05 * (moved / (1.0 - 0.9**10)) / (
                jnp.sqrt(squared / (1.0 - 0.95**10)) + 1e-08
            )
            fresh[0, :, cols] = weight[:, cols] - step

        @pl.when(slot >= hot)
        def _():
            fresh[0, :, cols] = weight[:, cols]
            fresh[1, :, cols] = moment[:, cols]
            fresh[2, :, cols] = second[:, cols]

    copies = [
        pltpu.make_async_copy(fresh.at[i], dst, sem.at[i])
        for i, dst in enumerate((w_hbm, m_hbm, s_hbm))
    ]
    for copy in copies:
        copy.start()
    for copy in copies:
        copy.wait()
    sq_out.wait()
    cold_out.wait()


def body(n, reps, features, out_grads, cold_sums, weight, moment, second, ranks):
    tokens, rows = features.shape
    width = out_grads.shape[1]
    blocks = ranks.shape[0]
    hot = blocks // 2
    packed = hot * LANES
    m = n // 2
    own = rows // n
    chunk = max(own, LANES)
    chunks = rows // chunk
    early, late, _ = split_rows(own)
    hops = max(bits_of(reps), 1)
    f32, bf16 = jnp.float32, jnp.bfloat16
    vmem = pl.BlockSpec(memory_space=pltpu.VMEM)
    smem = pl.BlockSpec(memory_space=pltpu.SMEM)
    hbm = pl.BlockSpec(memory_space=pl.ANY)
    dma = pltpu.SemaphoreType.DMA
    summed, sq, kept, w, mo, se = pl.pallas_call(
        functools.partial(exchange_kernel, n, reps, hot),
        out_shape=(
            pltpu.VMEM((own, packed), f32),
            pltpu.VMEM((blocks, LANES), f32),
            pltpu.VMEM(cold_sums.shape, bf16),
            pltpu.VMEM(weight.shape, f32),
            pltpu.VMEM(weight.shape, f32),
            pltpu.VMEM(weight.shape, f32),
        ),
        in_specs=[smem] + [pl.BlockSpec(memory_space=pltpu.HBM)] * 6,
        out_specs=(vmem,) * 6,
        scratch_shapes=[
            pltpu.VMEM((chunks, tokens, chunk), bf16),
            pltpu.VMEM((tokens, width), bf16),
            pltpu.VMEM((chunks, chunk, width), bf16),
            pltpu.VMEM((chunk, width), f32),
            pltpu.VMEM((n * early, packed), f32),
            pltpu.VMEM((m * early, packed), f32),
            pltpu.VMEM((m * early, packed), f32),
            pltpu.VMEM((m * early, packed), f32),
            pltpu.VMEM((m, 2 * late, packed), f32),
            pltpu.VMEM((late, packed), f32),
            pltpu.VMEM((m, 2 * late, packed), f32),
            pltpu.VMEM((m, 2 * late, packed), f32),
            pltpu.VMEM((hops + 1, blocks, LANES), f32),
            pltpu.VMEM((hops, blocks, LANES), f32),
            pltpu.VMEM((n, blocks, LANES), f32),
            dma((2, chunks)),
            dma((4,)),
            dma((m, SUB)),
            dma((m, SUB)),
            dma((m, SUB)),
            dma((m, SUB)),
            dma((m, SUB)),
            dma((hops,)),
            dma((hops,)),
            dma((n,)),
            dma((n,)),
            dma((m,)),
            dma((m,)),
            dma((m,)),
            dma,
            dma,
        ],
        compiler_params=pltpu.CompilerParams(
            collective_id=0, has_side_effects=True, vmem_limit_bytes=EXCHANGE_GRANT
        ),
        name="exchange",
    )(ranks, features, out_grads, cold_sums, weight, moment, second)
    new_weight, new_moment, new_second, new_cold, norms = pl.pallas_call(
        functools.partial(update_kernel, n, rows * reps, tokens, hot),
        out_shape=(
            jax.ShapeDtypeStruct(weight.shape, f32),
            jax.ShapeDtypeStruct(weight.shape, f32),
            jax.ShapeDtypeStruct(weight.shape, f32),
            jax.ShapeDtypeStruct(cold_sums.shape, bf16),
            jax.ShapeDtypeStruct((blocks, LANES), f32),
        ),
        in_specs=[smem] + [vmem] * 6,
        out_specs=(hbm,) * 5,
        scratch_shapes=[pltpu.VMEM((3,) + weight.shape, f32), dma, dma, dma((3,))],
        compiler_params=pltpu.CompilerParams(vmem_limit_bytes=VMEM_GRANT),
        name="update",
    )(ranks, summed, sq, kept, w, mo, se)
    return new_weight, new_moment, new_second, new_cold, norms.reshape(width)


def solution(mesh):
    owned = P(("rep", "dp"), None)
    placed = (P("dp", "rep"), P("dp", None), P("dp", "rep", None), owned, owned, owned, P())
    return jax.shard_map(
        functools.partial(body, mesh.shape["dp"], mesh.shape["rep"]),
        mesh=mesh,
        in_specs=placed,
        out_specs=(owned, owned, owned, P("dp", "rep", None), P()),
        check_vma=False,
    )
```
